32 devices in a mesh: rep: 4 (over y, x), tile: 8 (over z, core).
Axes of the slice: x: 2, y: 2, z: 4, core: 2. Of those that a mesh axis runs over, the one named last changes fastest.
Arguments:
- spins_in: float32 [4, 2048, 4096], P('rep', 'tile'), may hold values from -1 to 1
- noise: bfloat16 [2, 4, 2048, 4096], P(None, 'rep', 'tile'), may hold values from -1.5 to 1.5
- betas: float32 [4], replicated, as said below
- labels: int32 [4], P('rep'), may hold values from 0 to 3, each once
- accept: int32 [2, 4], P(None, 'rep'), may hold values 0 or 1
Outputs:
- spins: float32 [4, 2048, 4096], P('rep', 'tile')
- energy_rows: float32 [4, 2048], P('rep', 'tile')
- margin_rows: float32 [4, 2048], P('rep', 'tile')
- new_labels: int32 [4], P('rep')
- log_ratio: float32 [4], P('rep')
- new_beta: float32 [4], P('rep')
The draws below stay inside these ranges and needn't reach their ends.
Inputs may be any that keep to these rules, and one draw needn't show every extreme that they name: `labels`: a permutation of the temperature indices. `accept`: entry [p, r] is read only where r mod 2 equals p. `betas`: distinct and positive.
All inputs are finite; a program needn't handle non-finite values. No bound on the sum of `accept` on one device may be relied on, other than what follows from the above.
Results may differ from the reference program's by a relative error of at most 0.0003.
Values sent between devices are 32-bit elements; how exact they have to be, the bound alone decides.
A program may use at most 64 MiB of HBM per device.

```python
import jax
import jax.numpy as jnp
from jax import lax

COLS = 4096
SWEEPS = 2
ROWS = 2048
REPLICAS = 4


def draw_betas(key, part):
    steps = jnp.arange(REPLICAS, dtype=jnp.float32) / (REPLICAS - 1)
    ladder_values = 0.2 * jnp.exp(steps * jnp.log(5.0))
    jitter = jax.random.uniform(jax.random.fold_in(key, 11), (REPLICAS,), jnp.float32, 0.99, 1.01)
    return (ladder_values * jitter).astype(jnp.float32)


def touch_ends(array, rng, least, high):
    index_at = [jax.random.randint(jax.random.fold_in(rng, axis), (), 0, length) for axis, length in enumerate(array.shape)]
    longest = array.shape.index(max(array.shape))
    next_to = index_at[:longest] + [(index_at[longest] + 1) % array.shape[longest]] + index_at[longest + 1:]
    return array.at[tuple(index_at)].set(least).at[tuple(next_to)].set(high)


def steps_of(rng, extent, pieces, least, largest):
    factor_of = 1.0
    for dim, parts in pieces:
        heights = jax.random.uniform(jax.random.fold_in(jax.random.fold_in(rng, 6), dim), (parts,), jnp.float32, least / len(pieces), largest / len(pieces))
        factor_of = factor_of * jnp.repeat(jnp.exp(heights), extent[dim] // parts).reshape((-1,) + (1,) * (len(extent) - 1 - dim))
    return factor_of


def setup_inputs(seed: int = 0) -> dict:
    arg_keys = jax.random.split(jax.random.key(seed), 6)
    return {
        "spins_in": jnp.clip(jax.random.uniform(arg_keys[0], (REPLICAS, ROWS, COLS), jnp.float32, -1.0, 1.0) * steps_of(arg_keys[0], (REPLICAS, ROWS, COLS), ((0, 4), (1, 8)), -0.4, 0.0), -1.0, 1.0),
        "noise": jnp.clip(jax.random.uniform(arg_keys[1], (SWEEPS, REPLICAS, ROWS, COLS), jnp.float32, -1.5, 1.5) * steps_of(arg_keys[1], (SWEEPS, REPLICAS, ROWS, COLS), ((1, 4), (2, 8)), -0.4, 0.0), -1.5, 1.5).astype(jnp.bfloat16),
        "betas": draw_betas(jax.random.fold_in(arg_keys[5], 71), 0),
        "labels": jax.random.permutation(arg_keys[3], REPLICAS).astype(jnp.int32),
        "accept": touch_ends((jax.random.randint(arg_keys[4], (2, REPLICAS), 0, 2) < 1).astype(jnp.int32), jax.random.fold_in(arg_keys[4], 1), 0, 1),
    }


def ladder(energy, labels, accept, betas):
    count = energy.shape[0]
    slots = jnp.arange(count, dtype=jnp.int32)
    even = slots % 2 == 0
    accept_zero = accept[0]
    accept_one = accept[1]

    def beta_of(label_set):
        return jnp.sum(jnp.where(label_set[:, None] == slots[None, :], betas[None, :], 0.0), axis=1)

    e_next = jnp.roll(energy, -1)
    beta_zero = beta_of(labels)
    log_zero = (beta_zero - jnp.roll(beta_zero, -1)) * (energy - e_next)
    swap_zero = jnp.where(even, accept_zero, jnp.roll(accept_zero, 1))
    labels_one = jnp.where(swap_zero == 1, jnp.where(even, jnp.roll(labels, -1), jnp.roll(labels, 1)), labels)
    beta_one = beta_of(labels_one)
    log_one = (beta_one - jnp.roll(beta_one, -1)) * (energy - e_next)
    swap_one = jnp.where(even, jnp.roll(accept_one, 1), accept_one)
    labels_two = jnp.where(swap_one == 1, jnp.where(even, jnp.roll(labels_one, 1), jnp.roll(labels_one, -1)), labels_one)
    return labels_two.astype(jnp.int32), jnp.where(even, log_zero, log_one), beta_of(labels_two)


def sweep_one(lattice, noise_rep, beta):
    rows, cols = lattice.shape
    parity = (lax.broadcasted_iota(jnp.int32, (rows, cols), 0) + lax.broadcasted_iota(jnp.int32, (rows, cols), 1)) % 2
    for sweep in range(SWEEPS):
        for colour in range(2):
            field = jnp.roll(lattice, 1, 0) + jnp.roll(lattice, -1, 0) + jnp.roll(lattice, 1, 1) + jnp.roll(lattice, -1, 1)
            fresh = jnp.tanh(beta * field + noise_rep[sweep].astype(jnp.float32))
            lattice = jnp.where(parity == colour, fresh, lattice)
    bonds = jnp.roll(lattice, -1, 0) + jnp.roll(lattice, -1, 1)
    return lattice, -jnp.mean(lattice * bonds, axis=1)


def reference(spins_in, noise, betas, labels, accept):
    count = spins_in.shape[0]
    slots = jnp.arange(count, dtype=jnp.int32)

    def one_replica(index):
        beta = jnp.sum(jnp.where(slots == labels[index], betas, 0.0))
        return sweep_one(spins_in[index], noise[:, index], beta)

    spins, energy_rows = lax.map(one_replica, slots)

    def one_pair(index):
        partner = (index + 1) % count
        return jnp.mean(spins[index] * spins[partner], axis=1)

    margin_rows = lax.map(one_pair, slots)
    energy = jnp.mean(energy_rows, axis=1)
    new_labels, log_ratio, new_beta = ladder(energy, labels, accept, betas)
    return spins, energy_rows, margin_rows, new_labels, log_ratio, new_beta
```

```python
import functools

import jax
import jax.numpy as jnp
from jax import lax
from jax.experimental import pallas as pl
from jax.experimental.pallas import tpu as pltpu
from jax.sharding import PartitionSpec as P

SWEEPS = 2
STAGES = 2 * SWEEPS
H = 8
LANES = 128
ROWS = 2 * H
PAD = H
EARLY = 9
VMEM_BYTES = 60 * 1024 * 1024
MESH = pl.DeviceIdType.MESH


def kernel(
    n, peers, total_rows,
    spins_ref, noise_ref, betas_hbm, labels_hbm, accept_hbm,
    X, energy_ref, margin_ref, small_ref,
    SI, NB, NF, Q, R, EP, MP, MS, MR, EM, EG, LM, LG, betas_ref, labels_ref, accept_ref,
    s_sem, n_sem, hs_sem, hr_sem, bs_sem, br_sem,
    ms_sem, mr_sem, es_sem, er_sem, ls_sem, lr_sem, i_sem,
):
    T, C = spins_ref.shape[:2]
    rows, cols = T * H, C * LANES
    blocks = rows // ROWS
    half = C // 2
    me = lax.axis_index("rep")
    tile = lax.axis_index("tile")
    nxt = lax.rem(tile + 1, peers)
    prv = lax.rem(tile + peers - 1, peers)
    odd = lax.rem(me, 2)
    near = lax.rem(me + 1 + (n - 2) * odd, n)
    far = lax.rem(me + 2 + (n - 4) * odd, n)

    def load_spins(t):
        return pltpu.make_async_copy(
            spins_ref.at[t], SI.at[:, pl.ds(pl.multiple_of(PAD + t * H, H), H)], s_sem.at[t]
        )

    def load_noise(w, t):
        return pltpu.make_async_copy(noise_ref.at[w, t], NB.at[w, t], n_sem.at[w, t])

    def loaded(t):
        load_spins(t).wait()
        for w in range(SWEEPS):
            load_noise(w, t).wait()

    barrier = pltpu.get_barrier_semaphore()

    @pl.loop(1, peers)
    def _(d):
        pl.semaphore_signal(barrier, inc=1, device_id={"tile": lax.rem(tile + d, peers)}, device_id_type=MESH)

    @pl.loop(1, n)
    def _(d):
        pl.semaphore_signal(barrier, inc=1, device_id={"rep": lax.rem(me + d, n)}, device_id_type=MESH)

    small = [
        pltpu.make_async_copy(src, dst, i_sem.at[k])
        for k, (src, dst) in enumerate(
            ((betas_hbm, betas_ref), (labels_hbm, labels_ref), (accept_hbm, accept_ref))
        )
    ]
    for copy in small:
        copy.start()

    @pl.loop(0, T)
    def _(t):
        load_spins(t).start()
        for w in range(SWEEPS):
            load_noise(w, t).start()

    for copy in small:
        copy.wait()
    beta = jnp.float32(0.0)
    for k in range(n):
        beta = beta + jnp.where(labels_ref[0, 0] == k, betas_ref[k], 0.0)

    def halo_copies():
        copies = []
        for side, (start, slot, dev) in enumerate(((rows, 0, nxt), (PAD, PAD + rows, prv))):
            pairs = [(SI.at[:, pl.ds(start, H)], SI.at[:, pl.ds(slot, H)])]
            pairs += [(NF.at[w, :, pl.ds(start, H)], NF.at[w, :, pl.ds(slot, H)]) for w in range(SWEEPS)]
            for k, (src, dst) in enumerate(pairs):
                copies.append(
                    pltpu.make_async_remote_copy(
                        src, dst, hs_sem.at[side, k], hr_sem.at[side, k],
                        device_id={"tile": dev}, device_id_type=MESH,
                    )
                )
        return copies

    halos = halo_copies()

    def bulk(q, b):
        dest = lax.rem(me + (n - 2 + odd if q == 0 else 1 + odd), n)
        slot = 1 - odd if q == 0 else odd
        where = pl.ds(pl.multiple_of(b * ROWS, ROWS), ROWS)
        return pltpu.make_async_remote_copy(
            X.at[q * half : (q + 1) * half, where], R.at[slot, :, where],
            bs_sem.at[q, b], br_sem.at[slot, b],
            device_id={"rep": dest}, device_id_type=MESH,
        )

    def send(b):
        for q in range(2):
            bulk(q, b).start()

    def bulk_from(slot, b):
        where = pl.ds(pl.multiple_of(b * ROWS, ROWS), ROWS)
        return pltpu.make_async_remote_copy(
            X.at[0:half, where], R.at[slot, :, where], bs_sem.at[0, b], br_sem.at[slot, b],
            device_id={"rep": near}, device_id_type=MESH,
        )

    lane = lax.broadcasted_iota(jnp.int32, (H, LANES), 1)
    even = lax.rem(lane, 2) == 0
    first = lane == 0
    last = lane == LANES - 1

    def convert(t):
        where = pl.ds(pl.multiple_of(PAD + t * H, H), H)
        for w in range(SWEEPS):
            for c in range(C):
                NF[w, c, where, :] = NB[w, t, c].astype(jnp.float32)

    def strided(ref, index, start):
        return ref[(*index, pl.ds(start, H, stride=2), slice(None))]

    def stage(k, p):
        sweep, colour = k // 2, k % 2
        row = PAD + 2 * p

        def centre(c):
            if k:
                return Q[k - 1, c, pl.ds(PAD + p, H), :]
            return jnp.where(even, strided(SI, (c,), row + 1), strided(SI, (c,), row))

        def vertical(c):
            if k:
                before = Q[k - 1, c, pl.ds(PAD + p - 1, H), :]
                after = Q[k - 1, c, pl.ds(PAD + p + 1, H), :]
                return jnp.where(even, before, after) if colour == 0 else jnp.where(even, after, before)
            return jnp.where(even, strided(SI, (c,), row - 1), strided(SI, (c,), row + 2))

        def noise(c):
            upper, lower = strided(NF, (sweep, c), row), strided(NF, (sweep, c), row + 1)
            return jnp.where(even, upper, lower) if colour == 0 else jnp.where(even, lower, upper)

        here = centre(0)
        to_right = pltpu.roll(centre(C - 1), 1, 1)
        to_left = pltpu.roll(here, LANES - 1, 1)
        wrap = to_left
        for c in range(C):
            ahead = centre(c + 1) if c + 1 < C else None
            ahead_left = pltpu.roll(ahead, LANES - 1, 1) if c + 1 < C else wrap
            here_right = pltpu.roll(here, 1, 1)
            left = jnp.where(first, to_right, here_right)
            right = jnp.where(last, ahead_left, to_left)
            field = (here + vertical(c)) + (left + right)
            Q[k, c, pl.ds(PAD + p, H), :] = jnp.tanh(beta * field + noise(c))
            here, to_right, to_left = ahead, here_right, ahead_left

    def finish(b):
        p = pl.multiple_of(PAD + b * H, H)
        row = pl.multiple_of(b * ROWS, ROWS)
        for c in range(C):
            e, o = Q[2, c, pl.ds(p, H), :], Q[3, c, pl.ds(p, H), :]
            X[c, pl.ds(row, H, stride=2), :] = jnp.where(even, e, o)
            X[c, pl.ds(row + 1, H, stride=2), :] = jnp.where(even, o, e)

    def bonds(b):
        p = pl.multiple_of(PAD + b * H, H)
        row = pl.multiple_of(b * ROWS, ROWS)

        def pair(c):
            e, o = Q[2, c, pl.ds(p, H), :], Q[3, c, pl.ds(p, H), :]
            upper, lower = jnp.where(even, e, o), jnp.where(even, o, e)
            return upper, lower, pltpu.roll(upper, LANES - 1, 1), pltpu.roll(lower, LANES - 1, 1)

        here = pair(0)
        wrap = here
        total_upper = jnp.zeros((H, LANES), jnp.float32)
        total_lower = jnp.zeros((H, LANES), jnp.float32)
        for c in range(C):
            ahead = pair(c + 1) if c + 1 < C else wrap
            upper, lower, upper_left, lower_left = here
            below = jnp.where(even, Q[2, c, pl.ds(p + 1, H), :], Q[3, c, pl.ds(p + 1, H), :])
            total_upper = total_upper + upper * (lower + jnp.where(last, ahead[2], upper_left))
            total_lower = total_lower + lower * (below + jnp.where(last, ahead[3], lower_left))
            here = ahead
        EP[pl.ds(row, H, stride=2), :] = total_upper
        EP[pl.ds(row + 1, H, stride=2), :] = total_lower

    for t in range(4):
        loaded(t)
    convert(0)

    @pl.loop(0, blocks + 1)
    def _(s):
        final = s // blocks
        middle = 1 - final

        @pl.when((s >= 1) & (s < 3))
        def _():
            loaded(2 * s + 2)
            loaded(2 * s + 3)

        @pl.when(s == 3)
        def _():
            @pl.loop(8, T)
            def _(t):
                loaded(t)

        @pl.when(s < blocks - 1)
        def _():
            convert(2 * s + 1)
            convert(2 * s + 2)

        @pl.when(s == 4)
        def _():
            convert(T - 1)

        @pl.when(s == blocks - 1)
        def _():
            for copy in halos:
                copy.wait_recv()

        for k in range(STAGES):
            stage(k, middle * (s * H + STAGES - k) + final * (k - STAGES + 1))

        @pl.when(s == 1)
        def _():
            pl.semaphore_wait(barrier, n - 1 + peers - 1)

        @pl.when(s >= 1)
        def _():
            b = middle * s
            finish(b)
            bonds(b)

            @pl.when(s <= EARLY)
            def _():
                send(b)

        @pl.when(s == 4)
        def _():
            for copy in halos:
                copy.start()

    per_row = jnp.sum(EP[...].T, axis=0, keepdims=True) * (-1.0 / cols)
    energy_ref[...] = per_row
    local = jnp.broadcast_to(jnp.sum(per_row, axis=1, keepdims=True), (8, LANES))
    EM[...] = local
    EG[tile] = local

    def energy_copy(d):
        return pltpu.make_async_remote_copy(
            EM, EG.at[tile], es_sem.at[d], er_sem.at[tile],
            device_id={"tile": lax.rem(tile + d, peers)}, device_id_type=MESH,
        )

    def energy_from(d):
        src = lax.rem(tile + d, peers)
        return pltpu.make_async_remote_copy(
            EM, EG.at[src], es_sem.at[d], er_sem.at[src], device_id={"tile": src}, device_id_type=MESH
        )

    @pl.loop(1, peers)
    def _(d):
        energy_copy(d).start()

    @pl.loop(1, peers)
    def _(d):
        energy_from(d).wait_recv()

    energy = jnp.sum(EG[...], axis=0) / total_rows
    line = lax.broadcasted_iota(jnp.int32, (8, LANES), 0)
    label_float = labels_ref[0, 0].astype(jnp.float32)
    accept_zero = accept_ref[0, 0].astype(jnp.float32)
    accept_one = accept_ref[0, 1].astype(jnp.float32)
    message = jnp.where(
        line == 0, energy,
        jnp.where(line == 1, label_float, jnp.where(line == 2, accept_zero, accept_one)),
    )
    LM[...] = message
    LG[me] = message

    def ladder_copy(d):
        return pltpu.make_async_remote_copy(
            LM, LG.at[me], ls_sem.at[d], lr_sem.at[me],
            device_id={"rep": lax.rem(me + d, n)}, device_id_type=MESH,
        )

    def ladder_from(d):
        src = lax.rem(me + d, n)
        return pltpu.make_async_remote_copy(
            LM, LG.at[src], ls_sem.at[d], lr_sem.at[src], device_id={"rep": src}, device_id_type=MESH
        )

    @pl.loop(1, n)
    def _(d):
        ladder_copy(d).start()

    @pl.loop(EARLY + 1, blocks)
    def _(b):
        send(b)

    send(0)

    def margins(b):
        for slot in range(2):
            bulk_from(slot, b).wait_recv()
        for g in range(2):
            where = pl.ds(pl.multiple_of(b * ROWS + g * H, H), H)
            totals = [jnp.zeros((H, LANES), jnp.float32) for _ in range(2)]
            for c in range(half):
                own, one, two = X[odd * half + c, where, :], R[0, c, where, :], R[1, c, where, :]
                totals[0] = totals[0] + own * one
                totals[1] = totals[1] + one * two
            for q in range(2):
                MP[q, where, :] = totals[q]

    def margin_sums(start, stop):
        for q in range(2):
            sums = jnp.sum(MP[q, start:stop, :].T, axis=0, keepdims=True) * (1.0 / cols)
            MS[q, :, start:stop] = jnp.broadcast_to(sums, (8, stop - start))

    @pl.loop(1, blocks // 2)
    def _(b):
        margins(b)

    @pl.loop(1, n)
    def _(d):
        ladder_from(d).wait_recv()

    energies = [LG[r][0:1] for r in range(n)]
    labels = [LG[r][1:2] for r in range(n)]
    acc = [[LG[r][2 + p : 3 + p] for r in range(n)] for p in range(2)]

    def beta_of(label):
        value = jnp.zeros((1, LANES), jnp.float32)
        for k in range(n):
            value = value + jnp.where(label == float(k), betas_ref[k], 0.0)
        return value

    def swapped(current, accepts, start):
        result = list(current)
        for r in range(start, n, 2):
            o = (r + 1) % n
            take = accepts[r] == 1.0
            result[r] = jnp.where(take, current[o], current[r])
            result[o] = jnp.where(take, current[r], current[o])
        return result

    labels_one = swapped(labels, acc[0], 0)
    labels_two = swapped(labels_one, acc[1], 1)
    zero = [beta_of(x) for x in labels]
    one = [beta_of(x) for x in labels_one]
    two = [beta_of(x) for x in labels_two]
    my_label = jnp.zeros((1, LANES), jnp.float32)
    my_log = my_label
    my_beta = my_label
    for r in range(n):
        o = (r + 1) % n
        betas_here = zero if r % 2 == 0 else one
        log = (betas_here[r] - betas_here[o]) * (energies[r] - energies[o])
        my_label = jnp.where(me == r, labels_two[r], my_label)
        my_log = jnp.where(me == r, log, my_log)
        my_beta = jnp.where(me == r, two[r], my_beta)
    small_ref[...] = jnp.concatenate([my_label, my_log, my_beta, jnp.zeros((5, LANES), jnp.float32)], axis=0)

    @pl.loop(blocks // 2, blocks)
    def _(b):
        margins(b)

    margin_sums(rows // 2, rows)
    margins(0)
    margin_sums(0, rows // 2)

    home = pltpu.make_async_remote_copy(
        MS.at[1 - odd], MR.at[0], ms_sem.at[0], mr_sem.at[0], device_id={"rep": near}, device_id_type=MESH
    )
    away = pltpu.make_async_remote_copy(
        MS.at[1], MR.at[1], ms_sem.at[1], mr_sem.at[1], device_id={"rep": far}, device_id_type=MESH
    )
    home.start()

    @pl.when(odd == 1)
    def _():
        away.start()

    for copy in halos:
        copy.wait_send()

    @pl.loop(0, blocks)
    def _(b):
        for q in range(2):
            bulk(q, b).wait_send()

    @pl.loop(1, peers)
    def _(d):
        energy_copy(d).wait_send()

    @pl.loop(1, n)
    def _(d):
        ladder_copy(d).wait_send()

    home.wait()

    @pl.when(odd == 0)
    def _():
        margin_ref[...] = MS[0, 0:1, :] + MR[0, 0:1, :]

    @pl.when(odd == 1)
    def _():
        away.wait()
        margin_ref[...] = MR[0, 0:1, :] + MR[1, 0:1, :]


def settle(spins, energy, margin, small, *refs):
    spins_out, energy_out, margin_out, label_out, log_out, beta_out = refs[:6]
    label, log, beta, sem = refs[6:]
    T = spins_out.shape[0]
    pairs = [(energy, energy_out), (margin, margin_out)]
    pairs += [(spins.at[:, pl.ds(t * H, H)], spins_out.at[t]) for t in range(T)]
    pairs += [(label, label_out), (log, log_out), (beta, beta_out)]
    copies = [pltpu.make_async_copy(a, b, sem.at[k]) for k, (a, b) in enumerate(pairs)]
    for copy in copies[:-3]:
        copy.start()
    label[0] = jnp.max(small[0:1]).astype(jnp.int32)
    log[0] = jnp.max(small[1:2])
    beta[0] = jnp.max(small[2:3])
    for copy in copies[-3:]:
        copy.start()
    for copy in copies:
        copy.wait()


def body(n, peers, total_rows, spins_in, noise, betas, labels, accept):
    _, rows, cols = spins_in.shape
    T, C = rows // H, cols // LANES
    blocks = rows // ROWS
    f32 = jnp.float32
    limit = VMEM_BYTES - 4 * (rows * cols + 2 * rows + 8 * LANES)
    hbm = pl.BlockSpec(memory_space=pltpu.HBM)
    vmem = pl.BlockSpec(memory_space=pltpu.VMEM)
    dma = pltpu.SemaphoreType.DMA
    accept = jnp.transpose(accept)
    labels = labels.reshape(1, 1)
    spins_in = spins_in.reshape(T, H, C, LANES).transpose(0, 2, 1, 3)
    noise = noise.reshape(SWEEPS, T, H, C, LANES).transpose(0, 1, 3, 2, 4)
    results = pl.pallas_call(
        functools.partial(kernel, n, peers, total_rows),
        out_shape=(
            pltpu.VMEM((C, rows, LANES), f32),
            pltpu.VMEM((1, rows), f32),
            pltpu.VMEM((1, rows), f32),
            pltpu.VMEM((8, LANES), f32),
        ),
        in_specs=[hbm] * 5,
        out_specs=(vmem,) * 4,
        scratch_shapes=[
            pltpu.VMEM((C, rows + 3 * PAD, LANES), f32),
            pltpu.VMEM((SWEEPS, T, C, H, LANES), jnp.bfloat16),
            pltpu.VMEM((SWEEPS, C, rows + 3 * PAD, LANES), f32),
            pltpu.VMEM((STAGES, C, rows // 2 + 2 * PAD, LANES), f32),
            pltpu.VMEM((2, C // 2, rows, LANES), f32),
            pltpu.VMEM((rows, LANES), f32),
            pltpu.VMEM((2, rows, LANES), f32),
            pltpu.VMEM((2, 8, rows), f32),
            pltpu.VMEM((2, 8, rows), f32),
            pltpu.VMEM((8, LANES), f32),
            pltpu.VMEM((peers, 8, LANES), f32),
            pltpu.VMEM((8, LANES), f32),
            pltpu.VMEM((n, 8, LANES), f32),
            pltpu.SMEM(betas.shape, f32),
            pltpu.SMEM(labels.shape, jnp.int32),
            pltpu.SMEM(accept.shape, jnp.int32),
            dma((T,)),
            dma((SWEEPS, T)),
            dma((2, 1 + SWEEPS)),
            dma((2, 1 + SWEEPS)),
            dma((2, blocks)),
            dma((2, blocks)),
            dma((2,)),
            dma((2,)),
            dma((peers,)),
            dma((peers,)),
            dma((n,)),
            dma((n,)),
            dma((3,)),
        ],
        compiler_params=pltpu.CompilerParams(collective_id=0, has_side_effects=True, vmem_limit_bytes=limit),
        name="lattice_exchange",
    )(spins_in, noise, betas, labels, accept)
    out = pl.pallas_call(
        settle,
        out_shape=(
            jax.ShapeDtypeStruct(spins_in.shape, f32),
            jax.ShapeDtypeStruct((1, rows), f32),
            jax.ShapeDtypeStruct((1, rows), f32),
            jax.ShapeDtypeStruct((1,), jnp.int32),
            jax.ShapeDtypeStruct((1,), f32),
            jax.ShapeDtypeStruct((1,), f32),
        ),
        in_specs=[vmem] * 4,
        out_specs=(hbm,) * 6,
        scratch_shapes=[
            pltpu.SMEM((1,), jnp.int32),
            pltpu.SMEM((1,), f32),
            pltpu.SMEM((1,), f32),
            dma((T + 5,)),
        ],
        compiler_params=pltpu.CompilerParams(vmem_limit_bytes=VMEM_BYTES // 2),
        name="settle",
    )(*results)
    spins = out[0].transpose(0, 2, 1, 3).reshape(1, rows, cols)
    return (spins, *out[1:])


def solution(mesh):
    n = mesh.shape["rep"]
    peers = mesh.shape["tile"]
    in_specs = (P("rep", "tile", None), P(None, "rep", "tile", None), P(), P("rep"), P(None, "rep"))
    out_specs = (P("rep", "tile", None), P("rep", "tile"), P("rep", "tile"), P("rep"), P("rep"), P("rep"))

    def run(spins_in, noise, betas, labels, accept):
        total_rows = spins_in.shape[1]
        step = jax.shard_map(
            functools.partial(body, n, peers, total_rows),
            mesh=mesh, in_specs=in_specs, out_specs=out_specs, check_vma=False,
        )
        return step(spins_in, noise, betas, labels, accept)

    return run
```

```python
import functools

import jax
import jax.numpy as jnp
from jax import lax
from jax.experimental import pallas as pl
from jax.experimental.pallas import tpu as pltpu
from jax.sharding import PartitionSpec as P

SWEEPS = 2
STAGES = 2 * SWEEPS
H = 8
LANES = 128
ROWS = 2 * H
PAD = H
EARLY = 9
HALO = 6
PARTS = 4
SOON = 6
GATHER = 4
VMEM_BYTES = 60 * 1024 * 1024
MESH = pl.DeviceIdType.MESH


def kernel(
    n, peers, total_rows,
    spins_ref, noise_ref, betas_hbm, labels_hbm, accept_hbm,
    X, energy_ref, margin_ref, small_ref,
    G, NB, Q0, Q1, Q2, Q3, R, EP, MP, MS, MR, EM, EG, LM, LG, betas_ref, labels_ref, accept_ref,
    s_sem, n_sem, hs_sem, hr_sem, bs_sem, br_sem,
    ms_sem, mr_sem, es_sem, er_sem, ls_sem, lr_sem, i_sem, go_sem,
):
    T, C = spins_ref.shape[:2]
    rows, cols = T * H, C * LANES
    blocks = rows // ROWS
    half = C // 2
    me = lax.axis_index("rep")
    tile = lax.axis_index("tile")
    nxt = lax.rem(tile + 1, peers)
    prv = lax.rem(tile + peers - 1, peers)
    odd = lax.rem(me, 2)
    near = lax.rem(me + 1 + (n - 2) * odd, n)
    far = lax.rem(me + 2 + (n - 4) * odd, n)
    onward = lax.rem(me + n - 2 + 4 * odd, n)

    part = half // PARTS
    member = lax.rem((me + 1) // 2, 2)
    core = lax.rem(tile, 2)
    Q = (Q0, Q1, Q2, Q3)

    def load_spins(t, k):
        return pltpu.make_async_copy(
            spins_ref.at[t], G.at[0, :, pl.ds(pl.multiple_of(PAD + t * H, H), H)], s_sem.at[k]
        )

    def load_noise(w, start, stop, k):
        return pltpu.make_async_copy(noise_ref.at[w, start:stop], NB.at[w, start:stop], n_sem.at[w, k])

    def loaded(start, stop, k):
        pltpu.make_async_copy(spins_ref.at[start:stop], spins_ref.at[start:stop], s_sem.at[k]).wait()
        for w in range(SWEEPS):
            load_noise(w, start, stop, k).wait()

    small = [
        pltpu.make_async_copy(src, dst, i_sem.at[k])
        for k, (src, dst) in enumerate(
            ((betas_hbm, betas_ref), (labels_hbm, labels_ref), (accept_hbm, accept_ref))
        )
    ]
    for copy in small:
        copy.start()

    for w in range(SWEEPS):
        load_noise(w, 0, SOON, 0).start()
    for t in range(SOON):
        load_spins(t, 0).start()

    barrier = pltpu.get_barrier_semaphore()

    @pl.when(member == 1)
    def _():
        for peer in (near, onward):
            pl.semaphore_signal(barrier, inc=1, device_id={"rep": peer}, device_id_type=MESH)

    @pl.loop(1, peers)
    def _(d):
        pl.semaphore_signal(
            barrier, inc=1,
            device_id={"rep": me + (1 - member) * (near - me), "tile": lax.rem(tile + d, peers)}, device_id_type=MESH,
        )

    halos = [
        pltpu.make_async_remote_copy(
            G.at[:, :, pl.ds(start, H)], G.at[:, :, pl.ds(slot, H)], hs_sem.at[side], hr_sem.at[side],
            device_id={"tile": dev}, device_id_type=MESH,
        )
        for side, (start, slot, dev) in enumerate(((rows, 0, nxt), (PAD, PAD + rows, prv)))
    ]

    def bulk(q, b, start, width):
        dest = lax.rem(me + (n - 2 + odd if q == 0 else 1 + odd), n)
        slot = 1 - odd if q == 0 else odd
        where = pl.ds(pl.multiple_of(b * ROWS, ROWS), ROWS)
        group = (b // GATHER) if not isinstance(b, int) or b else blocks // GATHER
        return pltpu.make_async_remote_copy(
            X.at[pl.ds(q * half + start, width), where], R.at[pl.ds(slot * half + start, width), where],
            bs_sem, br_sem.at[group],
            device_id={"rep": dest}, device_id_type=MESH,
        )

    def send(b, start=0, width=half):
        for q in range(2):
            bulk(q, b, start, width).start()

    def gathered(start, stop, group):
        where = slice(start * ROWS, stop * ROWS)
        pltpu.make_async_remote_copy(
            X.at[:, where], R.at[:, where], bs_sem, br_sem.at[group],
            device_id={"rep": near}, device_id_type=MESH,
        ).wait_recv()

    lane = lax.broadcasted_iota(jnp.int32, (H, LANES), 1)
    even = lax.rem(lane, 2) == 0
    first = lane == 0
    last = lane == LANES - 1

    def convert(t, cs=range(C)):
        where = pl.ds(pl.multiple_of(PAD + t * H, H), H)
        for w in range(SWEEPS):
            for c in cs:
                G[1 + w, c, where, :] = NB[w, t, c].astype(jnp.float32)

    def strided(plane, c, start):
        return G[plane, c, pl.ds(start, H, stride=2), :]

    def stage(k, p, cs=range(C), ring=True):
        sweep, colour = k // 2, k % 2
        row = PAD + 2 * p

        def centre(c):
            if k:
                return Q[k - 1][c, pl.ds(PAD + p, H), :]
            return jnp.where(even, strided(0, c, row + 1), strided(0, c, row))

        def vertical(c):
            if k:
                before = Q[k - 1][c, pl.ds(PAD + p - 1, H), :]
                after = Q[k - 1][c, pl.ds(PAD + p + 1, H), :]
                return jnp.where(even, before, after) if colour == 0 else jnp.where(even, after, before)
            return jnp.where(even, strided(0, c, row - 1), strided(0, c, row + 2))

        def noise(c):
            upper, lower = strided(1 + sweep, c, row), strided(1 + sweep, c, row + 1)
            return jnp.where(even, upper, lower) if colour == 0 else jnp.where(even, lower, upper)

        def beside(c, d):
            return (c + d) % C

        count = len(cs)
        here = centre(cs[0])
        to_right = pltpu.roll(centre(cs[-1] if ring else beside(cs[0], -1)), 1, 1)
        to_left = pltpu.roll(here, LANES - 1, 1)
        wrap = to_left if ring else pltpu.roll(centre(beside(cs[-1], 1)), LANES - 1, 1)
        for i, c in enumerate(cs):
            ahead = centre(cs[i + 1]) if i + 1 < count else None
            ahead_left = pltpu.roll(ahead, LANES - 1, 1) if i + 1 < count else wrap
            here_right = pltpu.roll(here, 1, 1)
            left = jnp.where(first, to_right, here_right)
            right = jnp.where(last, ahead_left, to_left)
            field = (here + vertical(c)) + (left + right)
            Q[k][c, pl.ds(PAD + p, H), :] = jnp.tanh(beta * field + noise(c))
            here, to_right, to_left = ahead, here_right, ahead_left

    def finish(b, cs=range(C)):
        p = pl.multiple_of(PAD + b * H, H)
        row = pl.multiple_of(b * ROWS, ROWS)
        for c in cs:
            e, o = Q2[c, pl.ds(p, H), :], Q3[c, pl.ds(p, H), :]
            X[c, pl.ds(row, H, stride=2), :] = jnp.where(even, e, o)
            X[c, pl.ds(row + 1, H, stride=2), :] = jnp.where(even, o, e)

    def bonds(b):
        p = pl.multiple_of(PAD + b * H, H)
        row = pl.multiple_of(b * ROWS, ROWS)

        def pair(c):
            e, o = Q2[c, pl.ds(p, H), :], Q3[c, pl.ds(p, H), :]
            upper, lower = jnp.where(even, e, o), jnp.where(even, o, e)
            return upper, lower, pltpu.roll(upper, LANES - 1, 1), pltpu.roll(lower, LANES - 1, 1)

        here = pair(0)
        wrap = here
        total_upper = jnp.zeros((H, LANES), jnp.float32)
        total_lower = jnp.zeros((H, LANES), jnp.float32)
        for c in range(C):
            ahead = pair(c + 1) if c + 1 < C else wrap
            upper, lower, upper_left, lower_left = here
            below = jnp.where(even, Q2[c, pl.ds(p + 1, H), :], Q3[c, pl.ds(p + 1, H), :])
            total_upper = total_upper + upper * (lower + jnp.where(last, ahead[2], upper_left))
            total_lower = total_lower + lower * (below + jnp.where(last, ahead[3], lower_left))
            here = ahead
        EP[pl.ds(row, H, stride=2), :] = total_upper
        EP[pl.ds(row + 1, H, stride=2), :] = total_lower

    def forward():
        pl.semaphore_wait(barrier, 2)
        for peer in (near, onward):
            pl.semaphore_signal(go_sem.at[0], inc=1, device_id={"rep": peer}, device_id_type=MESH)

    @pl.when(me == n - 1)
    def _():
        forward()

    loaded(0, SOON, 0)

    for w in range(SWEEPS):
        load_noise(w, SOON, T, 1).start()

    @pl.loop(SOON, T)
    def _(t):
        load_spins(t, 1).start()

    for copy in small:
        copy.wait()
    beta = jnp.float32(0.0)
    for k in range(n):
        beta = beta + jnp.where(labels_ref[0, 0] == k, betas_ref[k], 0.0)

    def opening(low, high, index):
        spans = []
        for k in range(STAGES):
            reach = STAGES - 1 - k
            start, stop = low(reach), high(reach)
            spans.append([[(index + q * half + i) % C for i in range(start, stop)] for q in range(2)])
        for cs in spans[0]:
            for t in range(SOON - 1):
                convert(t, cs)
        for k in range(STAGES):
            for cs in spans[k]:
                for s in range(2):
                    stage(k, s * H + STAGES - k, cs, ring=False)
        for q in range(2):
            finish(1, [index + q * half + i for i in range(low(0), high(0))])

    opening(lambda reach: -reach, lambda reach: part + reach, 0)

    @pl.when(me == 0)
    def _():
        forward()

    @pl.when(member == 1)
    def _():
        pl.semaphore_wait(go_sem.at[0], 2)

    send(1, 0, part)
    opening(lambda reach: reach, lambda reach: half - part + reach, part)
    send(1, part, half - part)
    bonds(1)
    loaded(SOON, T, 1)

    @pl.loop(2, blocks + 1)
    def _(s):
        final = s // blocks
        middle = 1 - final

        @pl.when(s < blocks - 1)
        def _():
            convert(2 * s + 1)
            convert(2 * s + 2)

        @pl.when(s == HALO)
        def _():
            convert(T - 1)

            @pl.when(member == 1)
            def _():
                pl.semaphore_wait(barrier, 2 * (peers - 1))
                pl.semaphore_signal(go_sem.at[1], inc=1, device_id={"rep": near}, device_id_type=MESH)

            @pl.when(member == 0)
            def _():
                pl.semaphore_wait(go_sem.at[1], 1)

        @pl.when(s == blocks - 1)
        def _():
            for copy in halos:
                copy.wait_recv()

        for k in range(STAGES):
            stage(k, middle * (s * H + STAGES - k) + final * (k - STAGES + 1))

        b = middle * s
        finish(b)
        bonds(b)

        @pl.when(s <= EARLY)
        def _():
            send(s)

        @pl.when(s == HALO)
        def _():
            for copy in halos:
                copy.start()

    per_row = jnp.sum(EP[...].T, axis=0, keepdims=True) * (-1.0 / cols)
    energy_ref[...] = per_row
    local = jnp.broadcast_to(jnp.sum(per_row, axis=1, keepdims=True), (8, LANES))
    EM[...] = local
    EG[tile] = local

    def energy_copy(d):
        return pltpu.make_async_remote_copy(
            EM, EG.at[tile], es_sem, er_sem,
            device_id={"tile": lax.rem(tile + d, peers)}, device_id_type=MESH,
        )

    others = pltpu.make_async_remote_copy(
        EG.at[: peers - 1], EG.at[: peers - 1], es_sem, er_sem, device_id={"tile": nxt}, device_id_type=MESH
    )

    @pl.loop(1, peers)
    def _(d):
        energy_copy(d).start()

    others.wait_recv()

    energy = jnp.sum(EG[...], axis=0) / total_rows
    line = lax.broadcasted_iota(jnp.int32, (8, LANES), 0)
    label_float = labels_ref[0, 0].astype(jnp.float32)
    accept_zero = accept_ref[0, 0].astype(jnp.float32)
    accept_one = accept_ref[0, 1].astype(jnp.float32)
    message = jnp.where(
        line == 0, energy,
        jnp.where(line == 1, label_float, jnp.where(line == 2, accept_zero, accept_one)),
    )
    LM[...] = message
    LG[me] = message

    def ladder_copy(d):
        return pltpu.make_async_remote_copy(
            LM, LG.at[me], ls_sem, lr_sem,
            device_id={"rep": lax.rem(me + d, n)}, device_id_type=MESH,
        )

    rest = pltpu.make_async_remote_copy(
        LG.at[: n - 1], LG.at[: n - 1], ls_sem, lr_sem, device_id={"rep": near}, device_id_type=MESH
    )

    @pl.loop(1, n)
    def _(d):
        ladder_copy(d).start()

    @pl.loop(EARLY + 1, blocks)
    def _(b):
        send(b)

    @pl.when(core == 0)
    def _():
        send(0)

    def margins(b):
        for g in range(2):
            where = pl.ds(pl.multiple_of(b * ROWS + g * H, H), H)
            totals = [jnp.zeros((H, LANES), jnp.float32) for _ in range(2)]
            for c in range(half):
                own, one, two = X[odd * half + c, where, :], R[c, where, :], R[half + c, where, :]
                totals[0] = totals[0] + own * one
                totals[1] = totals[1] + one * two
            for q in range(2):
                MP[q, where, :] = totals[q]

    def margin_sums(start, stop):
        for q in range(2):
            sums = jnp.sum(MP[q, start:stop, :].T, axis=0, keepdims=True) * (1.0 / cols)
            MS[q, :, start:stop] = jnp.broadcast_to(sums, (8, stop - start))

    def collect(group):
        start, stop = max(1, group * GATHER), (group + 1) * GATHER
        gathered(start, stop, group)

        @pl.loop(start, stop)
        def _(b):
            margins(b)

    groups = blocks // GATHER
    for group in range(groups // 2):
        collect(group)

    rest.wait_recv()

    energies = [LG[r][0:1] for r in range(n)]
    labels = [LG[r][1:2] for r in range(n)]
    acc = [[LG[r][2 + p : 3 + p] for r in range(n)] for p in range(2)]

    def beta_of(label):
        value = jnp.zeros((1, LANES), jnp.float32)
        for k in range(n):
            value = value + jnp.where(label == float(k), betas_ref[k], 0.0)
        return value

    def swapped(current, accepts, start):
        result = list(current)
        for r in range(start, n, 2):
            o = (r + 1) % n
            take = accepts[r] == 1.0
            result[r] = jnp.where(take, current[o], current[r])
            result[o] = jnp.where(take, current[r], current[o])
        return result

    labels_one = swapped(labels, acc[0], 0)
    labels_two = swapped(labels_one, acc[1], 1)
    zero = [beta_of(x) for x in labels]
    one = [beta_of(x) for x in labels_one]
    two = [beta_of(x) for x in labels_two]
    my_label = jnp.zeros((1, LANES), jnp.float32)
    my_log = my_label
    my_beta = my_label
    for r in range(n):
        o = (r + 1) % n
        betas_here = zero if r % 2 == 0 else one
        log = (betas_here[r] - betas_here[o]) * (energies[r] - energies[o])
        my_label = jnp.where(me == r, labels_two[r], my_label)
        my_log = jnp.where(me == r, log, my_log)
        my_beta = jnp.where(me == r, two[r], my_beta)
    small_ref[...] = jnp.concatenate([my_label, my_log, my_beta, jnp.zeros((5, LANES), jnp.float32)], axis=0)

    for group in range(groups // 2, groups):
        collect(group)

    @pl.when(core == 1)
    def _():
        send(0)

    margin_sums(rows // 2, rows)
    gathered(0, 1, groups)
    margins(0)
    margin_sums(0, rows // 2)

    home = pltpu.make_async_remote_copy(
        MS.at[1 - odd], MR.at[0], ms_sem.at[0], mr_sem.at[0], device_id={"rep": near}, device_id_type=MESH
    )
    away = pltpu.make_async_remote_copy(
        MS.at[1], MR.at[1], ms_sem.at[1], mr_sem.at[1], device_id={"rep": far}, device_id_type=MESH
    )
    home.start()

    @pl.when(odd == 1)
    def _():
        away.start()

    for copy in halos:
        copy.wait_send()

    pltpu.make_async_remote_copy(
        X, R, bs_sem, br_sem.at[0], device_id={"rep": near}, device_id_type=MESH
    ).wait_send()
    others.wait_send()
    rest.wait_send()
    home.wait()

    @pl.when(odd == 0)
    def _():
        margin_ref[...] = MS[0, 0:1, :] + MR[0, 0:1, :]

    @pl.when(odd == 1)
    def _():
        away.wait()
        margin_ref[...] = MR[0, 0:1, :] + MR[1, 0:1, :]


def settle(spins, energy, margin, small, *refs):
    spins_out, energy_out, margin_out, label_out, log_out, beta_out = refs[:6]
    label, log, beta, sem = refs[6:]
    T = spins_out.shape[0]
    pairs = [(energy, energy_out), (margin, margin_out)]
    pairs += [(label, label_out), (log, log_out), (beta, beta_out)]
    copies = [pltpu.make_async_copy(a, b, sem.at[k]) for k, (a, b) in enumerate(pairs)]
    for t in range(T):
        pltpu.make_async_copy(spins.at[:, pl.ds(t * H, H)], spins_out.at[t], sem.at[5]).start()
    for copy in copies[:-3]:
        copy.start()
    label[0] = jnp.max(small[0:1]).astype(jnp.int32)
    log[0] = jnp.max(small[1:2])
    beta[0] = jnp.max(small[2:3])
    for copy in copies[-3:]:
        copy.start()
    for copy in copies:
        copy.wait()
    pltpu.make_async_copy(spins_out, spins_out, sem.at[5]).wait()


def body(n, peers, total_rows, spins_in, noise, betas, labels, accept):
    _, rows, cols = spins_in.shape
    T, C = rows // H, cols // LANES
    blocks = rows // ROWS
    f32 = jnp.float32
    limit = VMEM_BYTES - 4 * (rows * cols + 2 * rows + 8 * LANES)
    hbm = pl.BlockSpec(memory_space=pltpu.HBM)
    vmem = pl.BlockSpec(memory_space=pltpu.VMEM)
    dma = pltpu.SemaphoreType.DMA
    accept = jnp.transpose(accept)
    labels = labels.reshape(1, 1)
    spins_in = spins_in.reshape(T, H, C, LANES).transpose(0, 2, 1, 3)
    noise = noise.reshape(SWEEPS, T, H, C, LANES).transpose(0, 1, 3, 2, 4)
    results = pl.pallas_call(
        functools.partial(kernel, n, peers, total_rows),
        out_shape=(
            pltpu.VMEM((C, rows, LANES), f32),
            pltpu.VMEM((1, rows), f32),
            pltpu.VMEM((1, rows), f32),
            pltpu.VMEM((8, LANES), f32),
        ),
        in_specs=[hbm] * 5,
        out_specs=(vmem,) * 4,
        scratch_shapes=[
            pltpu.VMEM((1 + SWEEPS, C, rows + 3 * PAD, LANES), f32),
            pltpu.VMEM((SWEEPS, T, C, H, LANES), jnp.bfloat16),
            *[pltpu.VMEM((C, rows // 2 + 2 * PAD, LANES), f32) for _ in range(STAGES)],
            pltpu.VMEM((C, rows, LANES), f32),
            pltpu.VMEM((rows, LANES), f32),
            pltpu.VMEM((2, rows, LANES), f32),
            pltpu.VMEM((2, 8, rows), f32),
            pltpu.VMEM((2, 8, rows), f32),
            pltpu.VMEM((8, LANES), f32),
            pltpu.VMEM((peers, 8, LANES), f32),
            pltpu.VMEM((8, LANES), f32),
            pltpu.VMEM((n, 8, LANES), f32),
            pltpu.SMEM(betas.shape, f32),
            pltpu.SMEM(labels.shape, jnp.int32),
            pltpu.SMEM(accept.shape, jnp.int32),
            dma((2,)),
            dma((SWEEPS, 2)),
            dma((2,)),
            dma((2,)),
            dma,
            dma((blocks // GATHER + 1,)),
            dma((2,)),
            dma((2,)),
            dma,
            dma,
            dma,
            dma,
            dma((3,)),
            pltpu.SemaphoreType.REGULAR((2,)),
        ],
        compiler_params=pltpu.CompilerParams(collective_id=0, has_side_effects=True, vmem_limit_bytes=limit),
        name="lattice_exchange",
    )(spins_in, noise, betas, labels, accept)
    out = pl.pallas_call(
        settle,
        out_shape=(
            jax.ShapeDtypeStruct(spins_in.shape, f32),
            jax.ShapeDtypeStruct((1, rows), f32),
            jax.ShapeDtypeStruct((1, rows), f32),
            jax.ShapeDtypeStruct((1,), jnp.int32),
            jax.ShapeDtypeStruct((1,), f32),
            jax.ShapeDtypeStruct((1,), f32),
        ),
        in_specs=[vmem] * 4,
        out_specs=(hbm,) * 6,
        scratch_shapes=[
            pltpu.SMEM((1,), jnp.int32),
            pltpu.SMEM((1,), f32),
            pltpu.SMEM((1,), f32),
            dma((6,)),
        ],
        compiler_params=pltpu.CompilerParams(vmem_limit_bytes=VMEM_BYTES // 2),
        name="settle",
    )(*results)
    spins = out[0].transpose(0, 2, 1, 3).reshape(1, rows, cols)
    return (spins, *out[1:])


def solution(mesh):
    n = mesh.shape["rep"]
    peers = mesh.shape["tile"]
    in_specs = (P("rep", "tile", None), P(None, "rep", "tile", None), P(), P("rep"), P(None, "rep"))
    out_specs = (P("rep", "tile", None), P("rep", "tile"), P("rep", "tile"), P("rep"), P("rep"), P("rep"))

    def run(spins_in, noise, betas, labels, accept):
        total_rows = spins_in.shape[1]
        step = jax.shard_map(
            functools.partial(body, n, peers, total_rows),
            mesh=mesh, in_specs=in_specs, out_specs=out_specs, check_vma=False,
        )
        return step(spins_in, noise, betas, labels, accept)

    return run
```

```python
import functools

import jax
import jax.numpy as jnp
from jax import lax
from jax.experimental import pallas as pl
from jax.experimental.pallas import tpu as pltpu
from jax.sharding import PartitionSpec as P

SWEEPS = 2
STAGES = 2 * SWEEPS
H = 8
LANES = 128
ROWS = 2 * H
PAD = H
EARLY = 12
HALO = 6
SOON = 6
NEXT = 12
GATHER = 4
VMEM_BYTES = 60 * 1024 * 1024
MESH = pl.DeviceIdType.MESH


def kernel(
    n, peers, total_rows,
    spins_ref, noise_ref, betas_hbm, labels_hbm, accept_hbm,
    X, energy_ref, margin_ref, small_ref,
    G, NB, Q0, Q1, Q2, Q3, R, EP, MP, MS, MR, EM, EG, LM, LG, betas_ref, labels_ref, accept_ref,
    s_sem, n_sem, hs_sem, hr_sem, bs_sem, br_sem,
    ms_sem, mr_sem, es_sem, er_sem, ls_sem, lr_sem, i_sem, go_sem,
):
    T, C = spins_ref.shape[:2]
    rows, cols = T * H, C * LANES
    blocks = rows // ROWS
    half = C // 2
    me = lax.axis_index("rep")
    tile = lax.axis_index("tile")
    nxt = lax.rem(tile + 1, peers)
    prv = lax.rem(tile + peers - 1, peers)
    odd = lax.rem(me, 2)
    near = lax.rem(me + 1 + (n - 2) * odd, n)
    far = lax.rem(me + 2 + (n - 4) * odd, n)
    onward = lax.rem(me + n - 2 + 4 * odd, n)

    part = half // 2
    member = lax.rem((me + 1) // 2, 2)
    core = lax.rem(tile, 2)
    Q = (Q0, Q1, Q2, Q3)

    def load_spins(t, k):
        return pltpu.make_async_copy(
            spins_ref.at[t], G.at[0, :, pl.ds(pl.multiple_of(PAD + t * H, H), H)], s_sem.at[k]
        )

    def load_noise(w, start, stop, k):
        return pltpu.make_async_copy(noise_ref.at[w, start:stop], NB.at[w, start:stop], n_sem.at[k])

    def load(start, stop, k):
        for w in range(SWEEPS):
            load_noise(w, start, stop, k).start()

        @pl.loop(start, stop)
        def _(t):
            load_spins(t, k).start()

    def loaded(count, k):
        for ref, sem in ((spins_ref.at[:count], s_sem), (noise_ref.at[:, :count], n_sem)):
            pltpu.make_async_copy(ref, ref, sem.at[k]).wait()

    small = [
        pltpu.make_async_copy(src, dst, i_sem.at[k])
        for k, (src, dst) in enumerate(
            ((betas_hbm, betas_ref), (labels_hbm, labels_ref), (accept_hbm, accept_ref))
        )
    ]
    for copy in small:
        copy.start()

    for w in range(SWEEPS):
        load_noise(w, 1, SOON, 0).start()
    for t in range(1, SOON):
        load_spins(t, 0).start()

    barrier = pltpu.get_barrier_semaphore()

    @pl.when(member == 1)
    def _():
        for peer in (near, onward):
            pl.semaphore_signal(barrier, inc=1, device_id={"rep": peer}, device_id_type=MESH)

    @pl.loop(1, peers)
    def _(d):
        pl.semaphore_signal(
            barrier, inc=1,
            device_id={"rep": me + (1 - member) * (near - me), "tile": lax.rem(tile + d, peers)}, device_id_type=MESH,
        )

    halos = [
        pltpu.make_async_remote_copy(
            G.at[:, :, pl.ds(start, H)], G.at[:, :, pl.ds(slot, H)], hs_sem.at[side], hr_sem.at[side],
            device_id={"tile": dev}, device_id_type=MESH,
        )
        for side, (start, slot, dev) in enumerate(((rows, 0, nxt), (PAD, PAD + rows, prv)))
    ]

    groups = blocks // GATHER
    last_group = groups + 2

    def bulk(q, b, start, width):
        dest = lax.rem(me + (n - 2 + odd if q == 0 else 1 + odd), n)
        slot = 1 - odd if q == 0 else odd
        where = pl.ds(pl.multiple_of(b * ROWS, ROWS), ROWS)
        group = b // GATHER
        if isinstance(b, int) and b == 0:
            group = groups + slot
        elif isinstance(b, int) and b == blocks - 1:
            group = last_group
        return pltpu.make_async_remote_copy(
            X.at[pl.ds(q * half + start, width), where], R.at[pl.ds(slot * half + start, width), where],
            bs_sem, br_sem.at[group],
            device_id={"rep": dest}, device_id_type=MESH,
        )

    def send(b, start=0, width=half):
        for q in range(2):
            bulk(q, b, start, width).start()

    def gathered(start, stop, group, first=0, last=C):
        where = slice(start * ROWS, stop * ROWS)
        pltpu.make_async_remote_copy(
            X.at[first:last, where], R.at[first:last, where], bs_sem, br_sem.at[group],
            device_id={"rep": near}, device_id_type=MESH,
        ).wait_recv()

    lane = lax.broadcasted_iota(jnp.int32, (H, LANES), 1)
    even = lax.rem(lane, 2) == 0
    first = lane == 0
    last = lane == LANES - 1

    def convert(t, cs=range(C)):
        where = pl.ds(pl.multiple_of(PAD + t * H, H), H)
        for w in range(SWEEPS):
            for c in cs:
                G[1 + w, c, where, :] = NB[w, t, c].astype(jnp.float32)

    def strided(plane, c, start):
        return G[plane, c, pl.ds(start, H, stride=2), :]

    def stage(k, p, cs=range(C), ring=True):
        sweep, colour = k // 2, k % 2
        row = PAD + 2 * p

        def centre(c):
            if k:
                return Q[k - 1][c, pl.ds(PAD + p, H), :]
            return jnp.where(even, strided(0, c, row + 1), strided(0, c, row))

        def vertical(c):
            if k:
                before = Q[k - 1][c, pl.ds(PAD + p - 1, H), :]
                after = Q[k - 1][c, pl.ds(PAD + p + 1, H), :]
                return jnp.where(even, before, after) if colour == 0 else jnp.where(even, after, before)
            return jnp.where(even, strided(0, c, row - 1), strided(0, c, row + 2))

        def noise(c):
            upper, lower = strided(1 + sweep, c, row), strided(1 + sweep, c, row + 1)
            return jnp.where(even, upper, lower) if colour == 0 else jnp.where(even, lower, upper)

        def beside(c, d):
            return (c + d) % C

        count = len(cs)
        here = centre(cs[0])
        to_right = pltpu.roll(centre(cs[-1] if ring else beside(cs[0], -1)), 1, 1)
        to_left = pltpu.roll(here, LANES - 1, 1)
        wrap = to_left if ring else pltpu.roll(centre(beside(cs[-1], 1)), LANES - 1, 1)
        for i, c in enumerate(cs):
            ahead = centre(cs[i + 1]) if i + 1 < count else None
            ahead_left = pltpu.roll(ahead, LANES - 1, 1) if i + 1 < count else wrap
            here_right = pltpu.roll(here, 1, 1)
            left = jnp.where(first, to_right, here_right)
            right = jnp.where(last, ahead_left, to_left)
            field = (here + vertical(c)) + (left + right)
            Q[k][c, pl.ds(PAD + p, H), :] = jnp.tanh(beta * field + noise(c))
            here, to_right, to_left = ahead, here_right, ahead_left

    def finish(b, cs=range(C)):
        p = pl.multiple_of(PAD + b * H, H)
        row = pl.multiple_of(b * ROWS, ROWS)
        for c in cs:
            e, o = Q2[c, pl.ds(p, H), :], Q3[c, pl.ds(p, H), :]
            X[c, pl.ds(row, H, stride=2), :] = jnp.where(even, e, o)
            X[c, pl.ds(row + 1, H, stride=2), :] = jnp.where(even, o, e)

    def bonds(b):
        p = pl.multiple_of(PAD + b * H, H)
        row = pl.multiple_of(b * ROWS, ROWS)

        def pair(c):
            e, o = Q2[c, pl.ds(p, H), :], Q3[c, pl.ds(p, H), :]
            upper, lower = jnp.where(even, e, o), jnp.where(even, o, e)
            return upper, lower, pltpu.roll(upper, LANES - 1, 1), pltpu.roll(lower, LANES - 1, 1)

        here = pair(0)
        wrap = here
        total_upper = jnp.zeros((H, LANES), jnp.float32)
        total_lower = jnp.zeros((H, LANES), jnp.float32)
        for c in range(C):
            ahead = pair(c + 1) if c + 1 < C else wrap
            upper, lower, upper_left, lower_left = here
            below = jnp.where(even, Q2[c, pl.ds(p + 1, H), :], Q3[c, pl.ds(p + 1, H), :])
            total_upper = total_upper + upper * (lower + jnp.where(last, ahead[2], upper_left))
            total_lower = total_lower + lower * (below + jnp.where(last, ahead[3], lower_left))
            here = ahead
        EP[pl.ds(row, H, stride=2), :] = total_upper
        EP[pl.ds(row + 1, H, stride=2), :] = total_lower

    def forward():
        pl.semaphore_wait(barrier, 2)
        for peer in (near, onward):
            pl.semaphore_signal(go_sem.at[0], inc=1, device_id={"rep": peer}, device_id_type=MESH)

    @pl.when(me == n - 1)
    def _():
        forward()

    loaded(SOON - 1, 0)

    for copy in small:
        copy.wait()
    beta = jnp.float32(0.0)
    for k in range(n):
        beta = beta + jnp.where(labels_ref[0, 0] == k, betas_ref[k], 0.0)

    def opening(low, high, index):
        spans = []
        for k in range(STAGES):
            reach = STAGES - 1 - k
            start, stop = low(reach), high(reach)
            spans.append([[(index + q * half + i) % C for i in range(start, stop)] for q in range(2)])
        for cs in spans[0]:
            for t in range(1, SOON - 1):
                convert(t, cs)
        for k in range(STAGES):
            for cs in spans[k]:
                for s in range(2):
                    stage(k, s * H + STAGES - k, cs, ring=False)
        for q in range(2):
            finish(1, [index + q * half + i for i in range(low(0), high(0))])

    opening(lambda reach: -reach, lambda reach: part + reach, 0)

    @pl.when(me == 0)
    def _():
        forward()

    @pl.when(member == 1)
    def _():
        pl.semaphore_wait(go_sem.at[0], 2)

    send(1, 0, part)
    load(SOON, NEXT, 1)
    load(NEXT, T, 2)
    opening(lambda reach: reach, lambda reach: half - part + reach, part)
    send(1, part, half - part)
    load(0, 1, 2)
    bonds(1)
    loaded(NEXT - SOON, 1)

    @pl.loop(2, blocks + 1)
    def _(s):
        final = s // blocks
        middle = 1 - final

        @pl.when(2 * s + 2 == NEXT)
        def _():
            loaded(T + 1 - NEXT, 2)

        @pl.when(s < blocks - 1)
        def _():
            convert(2 * s + 1)
            convert(2 * s + 2)

        @pl.when(s == HALO)
        def _():
            convert(T - 1)
            convert(0)

            @pl.when(member == 1)
            def _():
                pl.semaphore_wait(barrier, 2 * (peers - 1))
                pl.semaphore_signal(go_sem.at[1], inc=1, device_id={"rep": near}, device_id_type=MESH)

            @pl.when(member == 0)
            def _():
                pl.semaphore_wait(go_sem.at[1], 1)

        @pl.when(s == blocks - 1)
        def _():
            for copy in halos:
                copy.wait_recv()

        for k in range(STAGES):
            stage(k, middle * (s * H + STAGES - k) + final * (k - STAGES + 1))

        b = middle * s
        finish(b)

        @pl.when(s <= EARLY)
        def _():
            send(s)

        bonds(b)

        @pl.when(s == HALO)
        def _():
            for copy in halos:
                copy.start()

    per_row = jnp.sum(EP[...].T, axis=0, keepdims=True) * (-1.0 / cols)
    energy_ref[...] = per_row
    local = jnp.broadcast_to(jnp.sum(per_row, axis=1, keepdims=True), (8, LANES))
    EM[...] = local
    EG[tile] = local

    def energy_copy(d):
        return pltpu.make_async_remote_copy(
            EM, EG.at[tile], es_sem, er_sem,
            device_id={"tile": lax.rem(tile + d, peers)}, device_id_type=MESH,
        )

    others = pltpu.make_async_remote_copy(
        EG.at[: peers - 1], EG.at[: peers - 1], es_sem, er_sem, device_id={"tile": nxt}, device_id_type=MESH
    )

    @pl.loop(1, peers)
    def _(d):
        energy_copy(d).start()

    others.wait_recv()

    energy = jnp.sum(EG[...], axis=0) / total_rows
    line = lax.broadcasted_iota(jnp.int32, (8, LANES), 0)
    label_float = labels_ref[0, 0].astype(jnp.float32)
    accept_zero = accept_ref[0, 0].astype(jnp.float32)
    accept_one = accept_ref[0, 1].astype(jnp.float32)
    message = jnp.where(
        line == 0, energy,
        jnp.where(line == 1, label_float, jnp.where(line == 2, accept_zero, accept_one)),
    )
    LM[...] = message
    LG[me] = message

    def ladder_copy(d):
        return pltpu.make_async_remote_copy(
            LM, LG.at[me], ls_sem, lr_sem,
            device_id={"rep": lax.rem(me + d, n)}, device_id_type=MESH,
        )

    rest = pltpu.make_async_remote_copy(
        LG.at[: n - 1], LG.at[: n - 1], ls_sem, lr_sem, device_id={"rep": near}, device_id_type=MESH
    )

    @pl.loop(1, n)
    def _(d):
        ladder_copy(d).start()

    @pl.loop(EARLY + 1, blocks - 1)
    def _(b):
        send(b)

    def close():
        send(blocks - 1)
        send(0)

    @pl.when(core == 0)
    def _():
        close()

    def margins(b, wanted=(0, 1)):
        for g in range(2):
            where = pl.ds(pl.multiple_of(b * ROWS + g * H, H), H)
            totals = [jnp.zeros((H, LANES), jnp.float32) for _ in range(2)]
            for c in range(half):
                one = R[c, where, :]
                if 0 in wanted:
                    totals[0] = totals[0] + X[odd * half + c, where, :] * one
                if 1 in wanted:
                    totals[1] = totals[1] + one * R[half + c, where, :]
            for q in wanted:
                MP[q, where, :] = totals[q]

    def margin_sums(start, stop, wanted=(0, 1)):
        for q in wanted:
            sums = jnp.sum(MP[q, start:stop, :].T, axis=0, keepdims=True) * (1.0 / cols)
            MS[q, :, start:stop] = jnp.broadcast_to(sums, (8, stop - start))

    def collect(group):
        start, stop = max(1, group * GATHER), min((group + 1) * GATHER, blocks - 1)
        gathered(start, stop, group)
        if group == groups - 1:
            @pl.when(core == 1)
            def _():
                close()

        @pl.loop(start, stop)
        def _(b):
            margins(b)

    for group in range(groups // 2):
        collect(group)

    rest.wait_recv()

    energies = [LG[r][0:1] for r in range(n)]
    labels = [LG[r][1:2] for r in range(n)]
    acc = [[LG[r][2 + p : 3 + p] for r in range(n)] for p in range(2)]

    def beta_of(label):
        value = jnp.zeros((1, LANES), jnp.float32)
        for k in range(n):
            value = value + jnp.where(label == float(k), betas_ref[k], 0.0)
        return value

    def swapped(current, accepts, start):
        result = list(current)
        for r in range(start, n, 2):
            o = (r + 1) % n
            take = accepts[r] == 1.0
            result[r] = jnp.where(take, current[o], current[r])
            result[o] = jnp.where(take, current[r], current[o])
        return result

    labels_one = swapped(labels, acc[0], 0)
    labels_two = swapped(labels_one, acc[1], 1)
    zero = [beta_of(x) for x in labels]
    one = [beta_of(x) for x in labels_one]
    two = [beta_of(x) for x in labels_two]
    my_label = jnp.zeros((1, LANES), jnp.float32)
    my_log = my_label
    my_beta = my_label
    for r in range(n):
        o = (r + 1) % n
        betas_here = zero if r % 2 == 0 else one
        log = (betas_here[r] - betas_here[o]) * (energies[r] - energies[o])
        my_label = jnp.where(me == r, labels_two[r], my_label)
        my_log = jnp.where(me == r, log, my_log)
        my_beta = jnp.where(me == r, two[r], my_beta)
    small_ref[...] = jnp.concatenate([my_label, my_log, my_beta, jnp.zeros((5, LANES), jnp.float32)], axis=0)

    for group in range(groups // 2, groups):
        collect(group)

    gathered(blocks - 1, blocks, last_group)
    margins(blocks - 1)
    margin_sums(rows // 2, rows)

    home = pltpu.make_async_remote_copy(
        MS.at[1 - odd], MR.at[0], ms_sem.at[0], mr_sem.at[0], device_id={"rep": near}, device_id_type=MESH
    )
    away = pltpu.make_async_remote_copy(
        MS.at[1], MR.at[1], ms_sem.at[1], mr_sem.at[1], device_id={"rep": far}, device_id_type=MESH
    )
    gathered(0, 1, groups, 0, half)
    margins(0, (0,))
    margin_sums(0, rows // 2, (0,))

    @pl.when(odd == 1)
    def _():
        home.start()

    gathered(0, 1, groups + 1, half, C)
    margins(0, (1,))
    margin_sums(0, rows // 2, (1,))

    @pl.when(odd == 0)
    def _():
        home.start()

    @pl.when(odd == 1)
    def _():
        away.start()

    for copy in halos:
        copy.wait_send()

    pltpu.make_async_remote_copy(
        X, R, bs_sem, br_sem.at[0], device_id={"rep": near}, device_id_type=MESH
    ).wait_send()
    others.wait_send()
    rest.wait_send()
    home.wait()

    @pl.when(odd == 0)
    def _():
        margin_ref[...] = MS[0, 0:1, :] + MR[0, 0:1, :]

    @pl.when(odd == 1)
    def _():
        away.wait()
        margin_ref[...] = MR[0, 0:1, :] + MR[1, 0:1, :]


def settle(spins, energy, margin, small, *refs):
    spins_out, energy_out, margin_out, label_out, log_out, beta_out = refs[:6]
    label, log, beta, sem = refs[6:]
    T = spins_out.shape[0]
    pairs = [(energy, energy_out), (margin, margin_out)]
    pairs += [(label, label_out), (log, log_out), (beta, beta_out)]
    copies = [pltpu.make_async_copy(a, b, sem.at[k]) for k, (a, b) in enumerate(pairs)]
    for t in range(T):
        pltpu.make_async_copy(spins.at[:, pl.ds(t * H, H)], spins_out.at[t], sem.at[5]).start()
    for copy in copies[:-3]:
        copy.start()
    label[0] = jnp.max(small[0:1]).astype(jnp.int32)
    log[0] = jnp.max(small[1:2])
    beta[0] = jnp.max(small[2:3])
    for copy in copies[-3:]:
        copy.start()
    for copy in copies:
        copy.wait()
    pltpu.make_async_copy(spins_out, spins_out, sem.at[5]).wait()


def body(n, peers, total_rows, spins_in, noise, betas, labels, accept):
    _, rows, cols = spins_in.shape
    T, C = rows // H, cols // LANES
    blocks = rows // ROWS
    f32 = jnp.float32
    limit = VMEM_BYTES - 4 * (rows * cols + 2 * rows + 8 * LANES)
    hbm = pl.BlockSpec(memory_space=pltpu.HBM)
    vmem = pl.BlockSpec(memory_space=pltpu.VMEM)
    dma = pltpu.SemaphoreType.DMA
    accept = jnp.transpose(accept)
    labels = labels.reshape(1, 1)
    spins_in = spins_in.reshape(T, H, C, LANES).transpose(0, 2, 1, 3)
    noise = noise.reshape(SWEEPS, T, H, C, LANES).transpose(0, 1, 3, 2, 4)
    results = pl.pallas_call(
        functools.partial(kernel, n, peers, total_rows),
        out_shape=(
            pltpu.VMEM((C, rows, LANES), f32),
            pltpu.VMEM((1, rows), f32),
            pltpu.VMEM((1, rows), f32),
            pltpu.VMEM((8, LANES), f32),
        ),
        in_specs=[hbm] * 5,
        out_specs=(vmem,) * 4,
        scratch_shapes=[
            pltpu.VMEM((1 + SWEEPS, C, rows + 3 * PAD, LANES), f32),
            pltpu.VMEM((SWEEPS, T, C, H, LANES), jnp.bfloat16),
            *[pltpu.VMEM((C, rows // 2 + 2 * PAD, LANES), f32) for _ in range(STAGES)],
            pltpu.VMEM((C, rows, LANES), f32),
            pltpu.VMEM((rows, LANES), f32),
            pltpu.VMEM((2, rows, LANES), f32),
            pltpu.VMEM((2, 8, rows), f32),
            pltpu.VMEM((2, 8, rows), f32),
            pltpu.VMEM((8, LANES), f32),
            pltpu.VMEM((peers, 8, LANES), f32),
            pltpu.VMEM((8, LANES), f32),
            pltpu.VMEM((n, 8, LANES), f32),
            pltpu.SMEM(betas.shape, f32),
            pltpu.SMEM(labels.shape, jnp.int32),
            pltpu.SMEM(accept.shape, jnp.int32),
            dma((3,)),
            dma((3,)),
            dma((2,)),
            dma((2,)),
            dma,
            dma((blocks // GATHER + 3,)),
            dma((2,)),
            dma((2,)),
            dma,
            dma,
            dma,
            dma,
            dma((3,)),
            pltpu.SemaphoreType.REGULAR((2,)),
        ],
        compiler_params=pltpu.CompilerParams(collective_id=0, has_side_effects=True, vmem_limit_bytes=limit),
        name="lattice_exchange",
    )(spins_in, noise, betas, labels, accept)
    out = pl.pallas_call(
        settle,
        out_shape=(
            jax.ShapeDtypeStruct(spins_in.shape, f32),
            jax.ShapeDtypeStruct((1, rows), f32),
            jax.ShapeDtypeStruct((1, rows), f32),
            jax.ShapeDtypeStruct((1,), jnp.int32),
            jax.ShapeDtypeStruct((1,), f32),
            jax.ShapeDtypeStruct((1,), f32),
        ),
        in_specs=[vmem] * 4,
        out_specs=(hbm,) * 6,
        scratch_shapes=[
            pltpu.SMEM((1,), jnp.int32),
            pltpu.SMEM((1,), f32),
            pltpu.SMEM((1,), f32),
            dma((6,)),
        ],
        compiler_params=pltpu.CompilerParams(vmem_limit_bytes=VMEM_BYTES // 2),
        name="settle",
    )(*results)
    spins = out[0].transpose(0, 2, 1, 3).reshape(1, rows, cols)
    return (spins, *out[1:])


def solution(mesh):
    n = mesh.shape["rep"]
    peers = mesh.shape["tile"]
    in_specs = (P("rep", "tile", None), P(None, "rep", "tile", None), P(), P("rep"), P(None, "rep"))
    out_specs = (P("rep", "tile", None), P("rep", "tile"), P("rep", "tile"), P("rep"), P("rep"), P("rep"))

    def run(spins_in, noise, betas, labels, accept):
        total_rows = spins_in.shape[1]
        step = jax.shard_map(
            functools.partial(body, n, peers, total_rows),
            mesh=mesh, in_specs=in_specs, out_specs=out_specs, check_vma=False,
        )
        return step(spins_in, noise, betas, labels, accept)

    return run
```
